32 devices in a mesh: vx: 4 (over y, x), vy: 8 (over z, core).
Axes of the slice: x: 2, y: 2, z: 4, core: 2. Of those that a mesh axis runs over, the one named last changes fastest.
Arguments:
- tokens: bfloat16 [96, 1, 256, 1024], P(('vx', 'vy')), may hold values from -256 to 256
- var_embed: bfloat16 [91, 1024], replicated, may hold values from -2 to 2
- query: bfloat16 [1024], replicated, may hold values from -6 to 6
- key_weight: bfloat16 [1024, 1024], P('vy'), may hold values from -1 to 1
- value_weight: bfloat16 [1024, 1024], P('vy'), may hold values from -0.1875 to 0.1875
- out_weight: bfloat16 [1024, 1024], P('vy'), may hold values from -0.1875 to 0.1875
- var_slot: int32 [91], replicated, may hold values from 0 to 95, as said below
Outputs:
- aggregated: bfloat16 [1, 256, 1024], P(None, ('vx', 'vy'))
The draws below stay inside these ranges and needn't reach their ends.
Inputs may be any that keep to these rules, and one draw needn't show every extreme that they name: `var_slot`: distinct slot numbers; at least one device's slot holds a variable.
All inputs are finite; a program needn't handle non-finite values.
Results may differ from the reference program's by a relative error of at most 0.0096.
Values may be sent and summed in bfloat16 or wider, within the bound.
A program may use at most 64 MiB of HBM per device.

```python
import math
import jax
import jax.numpy as jnp
from jax import lax

D = 1024
HEADS = 16
VARS = 91
B = 1
PATCH_DEV = 8
PATCH = 256
SLOT_DEV = 3
SLOTS = 96


def shared_params(key):
    first, second, third = jax.random.split(jax.random.fold_in(key, 7), 3)
    key_matrix = jax.random.truncated_normal(first, -6.0, 6.0, (D, D), jnp.float32) * D ** (-0.5)
    query_vector = jax.random.truncated_normal(second, -4.0, 4.0, (D,), jnp.float32) * 1.5
    embeddings = jax.random.truncated_normal(third, -4.0, 4.0, (VARS, D), jnp.float32) * 0.5
    return (key_matrix, query_vector, embeddings)


def slot_table(key):
    first, second, third = jax.random.split(jax.random.fold_in(key, 19), 3)
    ranking = jax.random.permutation(first, SLOTS).astype(jnp.int32)
    full_device = jax.random.randint(second, (), 0, SLOTS // SLOT_DEV)
    slot_index = jnp.arange(SLOTS, dtype=jnp.int32)
    priority = jnp.where(slot_index // SLOT_DEV == full_device, slot_index % SLOT_DEV - SLOT_DEV, ranking)
    ordering = jnp.argsort(priority, stable=True)
    occupied = ordering[:VARS]
    return occupied[jax.random.permutation(third, VARS)].astype(jnp.int32)


def draw_var_slot(key, part):
    return slot_table(key)


def draw_key_weight(key, part):
    return shared_params(key)[0].astype(jnp.bfloat16)


def draw_query(key, part):
    return shared_params(key)[1].astype(jnp.bfloat16)


def draw_var_embed(key, part):
    return shared_params(key)[2].astype(jnp.bfloat16)


def draw_tokens(key, part):
    keys_all = jax.random.split(jax.random.fold_in(key, 31), 1)
    return jax.random.truncated_normal(keys_all[0], -6.0, 6.0, (SLOTS, B, PATCH, D), jnp.float32).astype(jnp.bfloat16)


def steps_of(stream_key, extent, cuts, low, largest):
    def one(dim, parts):
        heights = jax.random.uniform(jax.random.fold_in(jax.random.fold_in(stream_key, 6), dim), (parts,), jnp.float32, low / len(cuts), largest / len(cuts))
        return jnp.repeat(jnp.exp(heights), extent[dim] // parts).reshape((-1,) + (1,) * (len(extent) - dim - 1))

    factor_of = one(*cuts[0])
    for cut in cuts[1:]:
        factor_of = factor_of * one(*cut)
    return factor_of


def bell_draw(rng, dims, deviation, reach, cuts=(), kind=jnp.bfloat16):
    array = deviation * jax.random.normal(rng, dims, jnp.float32)
    if cuts:
        array = array * steps_of(rng, dims, cuts, -0.22, 0.18)
    return jnp.clip(array, -reach, reach).astype(kind)


def setup_inputs(seed: int = 0) -> dict:
    key_list = jax.random.split(jax.random.key(seed), 8)
    return {
        "tokens": draw_tokens(jax.random.fold_in(key_list[7], 71), 0),
        "var_embed": draw_var_embed(jax.random.fold_in(key_list[7], 71), 0),
        "query": draw_query(jax.random.fold_in(key_list[7], 71), 0),
        "key_weight": draw_key_weight(jax.random.fold_in(key_list[7], 71), 0),
        "value_weight": bell_draw(key_list[4], (D, D), D ** -0.5, 0.1875, ((0, 8),)),
        "out_weight": bell_draw(key_list[5], (D, D), D ** -0.5, 0.1875, ((0, 8),)),
        "var_slot": draw_var_slot(jax.random.fold_in(key_list[7], 71), 0),
    }


def reference(tokens, var_embed, query, key_weight, value_weight, out_weight, var_slot):
    head_dim = D // HEADS
    scale = 1.0 / math.sqrt(head_dim)
    query_heads = query.astype(jnp.float32).reshape(HEADS, head_dim)
    embed_float = var_embed.astype(jnp.float32)

    def block(index):
        start = (index * PATCH_DEV).astype(jnp.int32)
        window = lax.dynamic_slice_in_dim(tokens, start, PATCH_DEV, 2)
        selected = jnp.take(window, var_slot.astype(jnp.int32), axis=0)
        mixed = (selected.astype(jnp.float32) + embed_float[:, None, None, :]).astype(jnp.bfloat16)
        flattened = mixed.reshape(-1, D)
        keys = jnp.dot(flattened.astype(jnp.float32), key_weight.astype(jnp.float32), preferred_element_type=jnp.float32).astype(jnp.bfloat16)
        values = jnp.dot(flattened.astype(jnp.float32), value_weight.astype(jnp.float32), preferred_element_type=jnp.float32).astype(jnp.bfloat16)
        keys = keys.reshape(VARS, B, PATCH_DEV, HEADS, head_dim)
        values = values.reshape(VARS, B, PATCH_DEV, HEADS, head_dim)
        scores = jnp.einsum('vbphe,he->vbph', keys.astype(jnp.float32), query_heads) * scale
        highest = lax.optimization_barrier(jnp.max(scores, axis=0, keepdims=True))
        exponent = jnp.exp(scores - highest)
        weights = (exponent / lax.optimization_barrier(jnp.sum(exponent, axis=0, keepdims=True))).astype(jnp.bfloat16)
        context = jnp.einsum('vbph,vbphe->bphe', weights.astype(jnp.float32), values.astype(jnp.float32))
        context = context.astype(jnp.bfloat16).reshape(B * PATCH_DEV, D)
        result = jnp.dot(context.astype(jnp.float32), out_weight.astype(jnp.float32), preferred_element_type=jnp.float32).astype(jnp.bfloat16)
        return result.reshape(B, PATCH_DEV, D)
    blocks = lax.map(block, jnp.arange(PATCH // PATCH_DEV, dtype=jnp.int32))
    return jnp.transpose(blocks, (1, 0, 2, 3)).reshape(B, PATCH, D)
```

```python
import functools
import math

import jax
import jax.numpy as jnp
from jax import lax
from jax.experimental import pallas as pl
from jax.experimental.pallas import tpu as pltpu
from jax.sharding import PartitionSpec as P

HEADS = 16
CORES = 2
LOWEST = -1e38
F32 = jnp.float32
BF16 = jnp.bfloat16
MESH = pl.DeviceIdType.MESH
NT = (((1,), (1,)), ((), ()))


def split(x):
    high = x.astype(BF16)
    return high, (x - high.astype(F32)).astype(BF16)


def dot(a, b):
    return jnp.dot(a, b, preferred_element_type=F32)


def kernel(nx, ny, heads, tok, emb, qry, wk, wv, wo, slot, out,
           mixed, wbuf, kq_mine, kq_in, kq_all, ex, stat, st_in, st2, st2_in, fexp,
           part, in1, p2, in2, o3, in3,
           kq_s, kq_r, w_s, w_r, st_s, st_r, st2_s, st2_r, s1_s, s1_r, s2_s, s2_r, s3_s, s3_r):
    slots, patches, width = tok.shape
    rows = width // ny
    na = ny // CORES
    group = patches // nx
    piece = width // nx
    own = patches // (nx * ny)
    hdim = width // heads
    scale = 1.0 / math.sqrt(hdim)
    i = lax.axis_index("vx")
    j = lax.axis_index("vy")
    a = j // CORES
    c = j % CORES
    me = i * CORES + c
    vx_peers = [lax.rem(i + d, nx) for d in range(1, nx)]
    a_peers = [lax.rem(a + d, na) for d in range(1, na)]
    vy_peers = [lax.rem(j + d, ny) for d in range(1, ny)]
    nplane = nx * CORES
    plane = [lax.rem(me + d, nplane) for d in range(1, nplane)]

    def remote(src, dst, ss, rs, x, y):
        return pltpu.make_async_remote_copy(
            src_ref=src, dst_ref=dst, send_sem=ss, recv_sem=rs,
            device_id=(x, y), device_id_type=MESH)

    sent = []

    def send(*args):
        copy = remote(*args)
        copy.start()
        sent.append(copy)

    def arrived(ref, ss, rs):
        remote(ref, ref, ss, rs, i, j).wait_recv()

    barrier = pltpu.get_barrier_semaphore()
    for y in vy_peers:
        pl.semaphore_signal(barrier, inc=1, device_id=(i, y), device_id_type=MESH)
    for x in vx_peers:
        for d in range(CORES):
            pl.semaphore_signal(barrier, inc=1, device_id=(x, a * CORES + d), device_id_type=MESH)

    head_row = lax.broadcasted_iota(jnp.int32, (heads, width), 0)
    head_col = lax.broadcasted_iota(jnp.int32, (heads, width), 1) // hdim
    qmat = jnp.where(head_row == head_col, jnp.broadcast_to(qry[...].astype(F32), (heads, width)), 0.0).astype(BF16)
    kq = lax.dot_general(qmat, wk[...], NT, preferred_element_type=F32)
    kq_high, kq_low = split(kq)
    kq_mine[0] = kq_high
    kq_mine[1] = kq_low

    pl.semaphore_wait(barrier, (ny - 1) + (nx - 1) * CORES)

    for y in vy_peers:
        send(kq_mine, kq_in.at[j], kq_s, kq_r.at[j], i, y)
    col_i = pl.ds(pl.multiple_of(i * piece, 128), piece)
    row_j = pl.ds(pl.multiple_of(j * rows, rows), rows)
    for x in a_peers:
        send(wv.at[:, col_i], wbuf.at[row_j, col_i], w_s, w_r.at[0, a, i], i, x * CORES + c)
    partner = a * CORES + (1 - c)
    send(wv, wbuf.at[row_j, :], w_s, w_r.at[1, a, 0], i, partner)

    wbuf[row_j, :] = wv[...]
    kq_in[j] = kq_mine[...]

    count = slot.shape[1]
    ids = (i * ny + j) * slots + lax.broadcasted_iota(jnp.int32, (8, count), 0)
    match = jnp.where(ids == jnp.broadcast_to(slot[...], (8, count)), 1.0, 0.0)
    held = jnp.max(match, axis=1, keepdims=True)
    embed = dot(match.astype(BF16), emb[...])
    for s in range(slots):
        mixed[s * patches:(s + 1) * patches, :] = (tok[s].astype(F32) + embed[s:s + 1, :]).astype(BF16)

    for y in vy_peers:
        arrived(kq_in.at[y], kq_s, kq_r.at[y])
    for y in range(ny):
        kq_all[:, :, y * rows:(y + 1) * rows] = kq_in[y]
    scores = []
    top = jnp.full((patches, heads), LOWEST, F32)
    for s in range(slots):
        block = mixed[s * patches:(s + 1) * patches, :]
        score = scale * (lax.dot_general(block, kq_all[0], NT, preferred_element_type=F32)
                         + lax.dot_general(block, kq_all[1], NT, preferred_element_type=F32))
        score = jnp.where(held[s:s + 1, :] > 0, score, LOWEST)
        scores.append(score)
        top = jnp.maximum(top, score)
    total = jnp.zeros((patches, heads), F32)
    for s in range(slots):
        e = jnp.where(held[s:s + 1, :] > 0, jnp.exp(scores[s] - top), 0.0).astype(BF16)
        ex[s * patches:(s + 1) * patches, :] = e
        total += e.astype(F32)
    stat[:, 0:heads] = top
    stat[:, heads:2 * heads] = total

    def group_rows(x):
        return pl.ds(pl.multiple_of(x * group, group), group)

    for p in plane:
        x = p // CORES
        send(stat.at[group_rows(x), :], st_in.at[me], st_s, st_r.at[me], x, a * CORES + p % CORES)
    st_in[me] = stat[group_rows(i), :]

    for x in a_peers:
        rws = pl.ds(pl.multiple_of((x * CORES + c) * rows, rows), rows)
        here = wbuf.at[rws, col_i]
        arrived(here, w_s, w_r.at[0, x, i])
        for q in vx_peers:
            send(here, here, w_s, w_r.at[0, x, i], q, j)
        send(here, here, w_s, w_r.at[1, x, i], i, partner)

    for p in plane:
        arrived(st_in.at[p], st_s, st_r.at[p])
    tops = [st_in[p][:, 0:heads] for p in range(nplane)]
    high = functools.reduce(jnp.maximum, tops)
    st2[:, 0:heads] = high
    st2[:, heads:2 * heads] = sum(
        jnp.exp(tops[p] - high) * st_in[p][:, heads:2 * heads] for p in range(nplane))
    for x in a_peers:
        send(st2, st2_in.at[a], st2_s, st2_r.at[a], i, x * CORES + c)
    st2_in[a] = st2[...]

    for x in a_peers:
        rws = pl.ds(pl.multiple_of((x * CORES + c) * rows, rows), rows)
        for q in vx_peers:
            here = wbuf.at[rws, pl.ds(pl.multiple_of(q * piece, 128), piece)]
            arrived(here, w_s, w_r.at[0, x, q])
            send(here, here, w_s, w_r.at[1, x, q], i, partner)

    for x in a_peers:
        arrived(st2_in.at[x], st2_s, st2_r.at[x])
    highest = functools.reduce(jnp.maximum, [st2_in[p][:, 0:heads] for p in range(na)])
    whole = sum(jnp.exp(st2_in[p][:, 0:heads] - highest) * st2_in[p][:, heads:2 * heads] for p in range(na))
    k = lax.broadcasted_iota(jnp.int32, (heads, na * rows), 1)
    feature = ((k // rows) * CORES + c) * rows + k % rows
    spread = jnp.where(feature // hdim == lax.broadcasted_iota(jnp.int32, (heads, na * rows), 0), 1.0, 0.0).astype(BF16)
    for p in range(nplane):
        factor = jnp.exp(st_in[p][:, 0:heads] - highest) / whole
        f_high, f_low = split(factor)
        grown = dot(f_high, spread) + dot(f_low, spread)
        for x in range(na):
            fexp[x, p] = grown[:, x * rows:(x + 1) * rows]

    arrived(wbuf.at[pl.ds(pl.multiple_of(partner * rows, rows), rows), :], w_s, w_r.at[1, a, 0])
    for x in a_peers:
        rws = pl.ds(pl.multiple_of((x * CORES + 1 - c) * rows, rows), rows)
        for q in range(nx):
            arrived(wbuf.at[rws, q * piece:(q + 1) * piece], w_s, w_r.at[1, x, q])

    order = a_peers + [a]

    def project(x):
        wide = CORES * rows
        start = pl.multiple_of(x * wide, wide)
        col = start + lax.broadcasted_iota(jnp.int32, (heads, wide), 1)
        to_cols = jnp.where(col // hdim == lax.broadcasted_iota(jnp.int32, (heads, wide), 0), 1.0, 0.0).astype(BF16)
        value = dot(mixed[...], wbuf[:, pl.ds(start, wide)])
        value = value * dot(ex[...], to_cols)
        context = sum(value[s * patches:(s + 1) * patches] for s in range(slots)).astype(BF16)
        for g in range(nx):
            for d in range(CORES):
                part[x, g * CORES + d] = context[g * group:(g + 1) * group, d * rows:(d + 1) * rows]
        for p in plane:
            send(part.at[x, p], in1.at[x, me], s1_s, s1_r.at[x, me], p // CORES, a * CORES + p % CORES)

    def combine(x, last):
        for p in plane:
            arrived(in1.at[x, p], s1_s, s1_r.at[x, p])
        acc = fexp[x, me] * part[x, me].astype(F32)
        for p in plane:
            acc += fexp[x, p] * in1[x, p].astype(F32)
        if last:
            return acc
        p2[x] = acc.astype(BF16)
        send(p2.at[x], in2.at[a], s2_s, s2_r.at[a], i, x * CORES + c)

    project(order[0])
    for n in range(1, na):
        project(order[n])
        combine(order[n - 1], False)
    acc = combine(a, True)
    for x in a_peers:
        arrived(in2.at[x], s2_s, s2_r.at[x])
        acc += in2[x].astype(F32)
    result = dot(acc.astype(BF16), wo[...]).astype(BF16)
    for y in range(ny):
        o3[y] = result[y * own:(y + 1) * own]
    for y in vy_peers:
        send(o3.at[y], in3.at[j], s3_s, s3_r.at[j], i, y)
    final = o3[j].astype(F32)
    for y in vy_peers:
        arrived(in3.at[y], s3_s, s3_r.at[y])
        final += in3[y].astype(F32)
    out[...] = final.astype(BF16)
    for copy in sent:
        copy.wait_send()


def shards(tokens, var_embed, query, key_weight, value_weight, out_weight, var_slot):
    slots, batch, patches, width = tokens.shape
    nx, ny = lax.axis_size("vx"), lax.axis_size("vy")
    heads = HEADS
    rows, na, group, own = width // ny, ny // CORES, patches // nx, patches // (nx * ny)
    nplane = nx * CORES
    dma = pltpu.SemaphoreType.DMA
    vmem = pltpu.VMEM
    result = pl.pallas_call(
        functools.partial(kernel, nx, ny, heads),
        out_shape=jax.ShapeDtypeStruct((own, width), BF16),
        in_specs=[pl.BlockSpec(memory_space=pltpu.VMEM)] * 7,
        out_specs=pl.BlockSpec(memory_space=pltpu.VMEM),
        scratch_shapes=[
            vmem((slots * patches, width), BF16),
            vmem((width, width), BF16),
            vmem((2, heads, rows), BF16),
            vmem((ny, 2, heads, rows), BF16),
            vmem((2, heads, width), BF16),
            vmem((slots * patches, heads), BF16),
            vmem((patches, 2 * heads), F32),
            vmem((nplane, group, 2 * heads), F32),
            vmem((group, 2 * heads), F32),
            vmem((na, group, 2 * heads), F32),
            vmem((na, nplane, group, rows), F32),
            vmem((na, nplane, group, rows), BF16),
            vmem((na, nplane, group, rows), BF16),
            vmem((na, group, rows), BF16),
            vmem((na, group, rows), BF16),
            vmem((ny, own, width), BF16),
            vmem((ny, own, width), BF16),
            dma, dma((ny,)),
            dma, dma((2, na, nx)),
            dma, dma((nplane,)),
            dma, dma((na,)),
            dma, dma((na, nplane)),
            dma, dma((na,)),
            dma, dma((ny,)),
        ],
        compiler_params=pltpu.CompilerParams(
            collective_id=0, has_side_effects=True, vmem_limit_bytes=60 * 1024 * 1024),
    )(
        tokens.reshape(slots, batch * patches, width), var_embed, query.reshape(1, width),
        key_weight, value_weight, out_weight, var_slot.reshape(1, -1),
    )
    return result.reshape(batch, -1, width)


def solution(mesh):
    placed = (
        P(("vx", "vy"), None, None, None),
        P(),
        P(),
        P("vy", None),
        P("vy", None),
        P("vy", None),
        P(),
    )
    return jax.shard_map(
        shards, mesh=mesh, in_specs=placed, out_specs=P(None, ("vx", "vy"), None), check_vma=False
    )
```

```python
import functools
import math

import jax
import jax.numpy as jnp
from jax import lax
from jax.experimental import pallas as pl
from jax.experimental.pallas import tpu as pltpu
from jax.sharding import PartitionSpec as P

HEADS = 16
CORES = 2
LOWEST = -1e38
F32 = jnp.float32
BF16 = jnp.bfloat16
MESH = pl.DeviceIdType.MESH
NT = (((1,), (1,)), ((), ()))


def split(x):
    high = x.astype(BF16)
    return high, (x - high.astype(F32)).astype(BF16)


def dot(a, b):
    return jnp.dot(a, b, preferred_element_type=F32)


def kernel(nx, ny, heads, tok_any, emb_any, qry_any, wk_any, wv_any, wo_any, slot_any, out,
           tok, emb, qry, wk, wo, slot, load_s,
           mixed, wbuf, kq_mine, kq_in, kq_all, ex, stat, st_in, st2, st2_in, fexp,
           part, in1, p2, in2, o3, in3,
           kq_s, kq_r, w_s, w_r, wp_s, wp_r, st_s, st_r, st2_s, st2_r, s1_s, s1_r, s2_s, s2_r, s3_s, s3_r):
    slots, patches, width = tok.shape
    rows = width // ny
    na = ny // CORES
    group = patches // nx
    piece = rows // nx
    wide = CORES * rows
    own = patches // (nx * ny)
    hdim = width // heads
    scale = 1.0 / math.sqrt(hdim)
    i = lax.axis_index("vx")
    j = lax.axis_index("vy")
    a = j // CORES
    c = j % CORES
    me = i * CORES + c
    vx_peers = [lax.rem(i + d, nx) for d in range(1, nx)]
    a_peers = [lax.rem(a + d, na) for d in range(1, na)]
    vy_peers = [lax.rem(j + d, ny) for d in range(1, ny)]
    nplane = nx * CORES
    plane = [lax.rem(me + d, nplane) for d in range(1, nplane)]

    def remote(src, dst, ss, rs, x, y):
        return pltpu.make_async_remote_copy(
            src_ref=src, dst_ref=dst, send_sem=ss, recv_sem=rs,
            device_id=(x, y), device_id_type=MESH)

    sent = []

    def send(*args):
        copy = remote(*args)
        copy.start()
        sent.append(copy)

    def arrived(ref, ss, rs):
        remote(ref, ref, ss, rs, i, j).wait_recv()

    row_j = pl.ds(pl.multiple_of(j * rows, rows), rows)
    pairs = ((wk_any, wk), (qry_any, qry), (wv_any, wbuf.at[row_j, :]), (tok_any, tok),
             (emb_any, emb), (slot_any, slot), (wo_any, wo))
    loads = [pltpu.make_async_copy(src, dst, load_s.at[n]) for n, (src, dst) in enumerate(pairs)]
    for load in loads:
        load.start()

    barrier = pltpu.get_barrier_semaphore()
    for y in vy_peers:
        pl.semaphore_signal(barrier, inc=1, device_id=(i, y), device_id_type=MESH)
    for x in vx_peers:
        for d in range(CORES):
            pl.semaphore_signal(barrier, inc=1, device_id=(x, a * CORES + d), device_id_type=MESH)

    loads[0].wait()
    loads[1].wait()
    head_row = lax.broadcasted_iota(jnp.int32, (heads, width), 0)
    head_col = lax.broadcasted_iota(jnp.int32, (heads, width), 1) // hdim
    qmat = jnp.where(head_row == head_col, jnp.broadcast_to(qry[...].astype(F32).reshape(1, width), (heads, width)), 0.0).astype(BF16)
    kq = lax.dot_general(qmat, wk[...], NT, preferred_element_type=F32)
    kq_high, kq_low = split(kq)
    kq_mine[0] = kq_high
    kq_mine[1] = kq_low

    pl.semaphore_wait(barrier, (ny - 1) + (nx - 1) * CORES)

    for y in vy_peers:
        send(kq_mine, kq_in.at[j], kq_s, kq_r.at[j], i, y)

    def block(x, d, q, n):
        first = pl.multiple_of((x * CORES + d) * rows + q * piece, piece)
        return wbuf.at[pl.ds(first, piece), pl.ds(pl.multiple_of(n * wide, wide), wide)]

    def turn(x, step):
        return lax.rem(x + 1 + step, na)

    partner = a * CORES + (1 - c)
    loads[2].wait()
    for step in range(na):
        for x in a_peers:
            n = turn(x, step)
            send(block(a, c, i, n), block(a, c, i, n), w_s, w_r.at[0, a, i, n], i, x * CORES + c)
    send(wbuf.at[row_j, :], wbuf.at[row_j, :], wp_s, wp_r, i, partner)

    kq_in[j] = kq_mine[...]

    for load in loads[3:]:
        load.wait()
    count = slot.shape[1]
    ids = (i * ny + j) * slots + lax.broadcasted_iota(jnp.int32, (8, count), 0)
    match = jnp.where(ids == jnp.broadcast_to(slot[...], (8, count)), 1.0, 0.0)
    held = jnp.max(match, axis=1, keepdims=True)
    embed = dot(match.astype(BF16), emb[...])
    for s in range(slots):
        mixed[s * patches:(s + 1) * patches, :] = (tok[s].astype(F32) + embed[s:s + 1, :]).astype(BF16)

    for y in vy_peers:
        arrived(kq_in.at[y], kq_s, kq_r.at[y])
    for y in range(ny):
        kq_all[:, :, y * rows:(y + 1) * rows] = kq_in[y]
    scores = []
    top = jnp.full((patches, heads), LOWEST, F32)
    for s in range(slots):
        rows_s = mixed[s * patches:(s + 1) * patches, :]
        score = scale * (lax.dot_general(rows_s, kq_all[0], NT, preferred_element_type=F32)
                         + lax.dot_general(rows_s, kq_all[1], NT, preferred_element_type=F32))
        score = jnp.where(held[s:s + 1, :] > 0, score, LOWEST)
        scores.append(score)
        top = jnp.maximum(top, score)
    total = jnp.zeros((patches, heads), F32)
    for s in range(slots):
        e = jnp.where(held[s:s + 1, :] > 0, jnp.exp(scores[s] - top), 0.0).astype(BF16)
        ex[s * patches:(s + 1) * patches, :] = e
        total += e.astype(F32)
    stat[:, 0:heads] = top
    stat[:, heads:2 * heads] = total

    def group_rows(x):
        return pl.ds(pl.multiple_of(x * group, group), group)

    for p in plane:
        x = p // CORES
        send(stat.at[group_rows(x), :], st_in.at[me], st_s, st_r.at[me], x, a * CORES + p % CORES)
    st_in[me] = stat[group_rows(i), :]

    def share(step):
        n = turn(a, step)
        for x in a_peers:
            here = block(x, c, i, n)
            arrived(here, w_s, w_r.at[0, x, i, n])
            for q in vx_peers:
                send(here, here, w_s, w_r.at[0, x, i, n], q, j)
            send(here, here, w_s, w_r.at[1, x, i, n], i, partner)

    def hand_over(step):
        n = turn(a, step)
        for x in a_peers:
            for q in vx_peers:
                here = block(x, c, q, n)
                arrived(here, w_s, w_r.at[0, x, q, n])
                send(here, here, w_s, w_r.at[1, x, q, n], i, partner)

    def complete(step):
        n = turn(a, step)
        for x in a_peers:
            for q in range(nx):
                arrived(block(x, 1 - c, q, n), w_s, w_r.at[1, x, q, n])

    share(0)
    if na > 1:
        share(1)
    hand_over(0)

    for p in plane:
        arrived(st_in.at[p], st_s, st_r.at[p])
    tops = [st_in[p][:, 0:heads] for p in range(nplane)]
    high = functools.reduce(jnp.maximum, tops)
    st2[:, 0:heads] = high
    st2[:, heads:2 * heads] = sum(
        jnp.exp(tops[p] - high) * st_in[p][:, heads:2 * heads] for p in range(nplane))
    for x in a_peers:
        send(st2, st2_in.at[a], st2_s, st2_r.at[a], i, x * CORES + c)
    st2_in[a] = st2[...]

    order = a_peers + [a]

    def project(x):
        start = pl.multiple_of(x * wide, wide)
        col = start + lax.broadcasted_iota(jnp.int32, (heads, wide), 1)
        to_cols = jnp.where(col // hdim == lax.broadcasted_iota(jnp.int32, (heads, wide), 0), 1.0, 0.0).astype(BF16)
        value = dot(mixed[...], wbuf[:, pl.ds(start, wide)])
        value = value * dot(ex[...], to_cols)
        context = sum(value[s * patches:(s + 1) * patches] for s in range(slots)).astype(BF16)
        for g in range(nx):
            for d in range(CORES):
                part[x, g * CORES + d] = context[g * group:(g + 1) * group, d * rows:(d + 1) * rows]
        for p in plane:
            send(part.at[x, p], in1.at[x, me], s1_s, s1_r.at[x, me], p // CORES, a * CORES + p % CORES)

    def combine(x, last):
        for p in plane:
            arrived(in1.at[x, p], s1_s, s1_r.at[x, p])
        acc = fexp[x, me] * part[x, me].astype(F32)
        for p in plane:
            acc += fexp[x, p] * in1[x, p].astype(F32)
        if last:
            return acc
        p2[x] = acc.astype(BF16)
        send(p2.at[x], in2.at[a], s2_s, s2_r.at[a], i, x * CORES + c)

    arrived(wbuf.at[pl.ds(pl.multiple_of(partner * rows, rows), rows), :], wp_s, wp_r)
    complete(0)
    project(order[0])
    if na > 2:
        share(2)
    if na > 1:
        hand_over(1)

    for x in a_peers:
        arrived(st2_in.at[x], st2_s, st2_r.at[x])
    highest = functools.reduce(jnp.maximum, [st2_in[p][:, 0:heads] for p in range(na)])
    whole = sum(jnp.exp(st2_in[p][:, 0:heads] - highest) * st2_in[p][:, heads:2 * heads] for p in range(na))
    k = lax.broadcasted_iota(jnp.int32, (heads, na * rows), 1)
    feature = ((k // rows) * CORES + c) * rows + k % rows
    spread = jnp.where(feature // hdim == lax.broadcasted_iota(jnp.int32, (heads, na * rows), 0), 1.0, 0.0).astype(BF16)
    for p in range(nplane):
        factor = jnp.exp(st_in[p][:, 0:heads] - highest) / whole
        f_high, f_low = split(factor)
        grown = dot(f_high, spread) + dot(f_low, spread)
        for x in range(na):
            fexp[x, p] = grown[:, x * rows:(x + 1) * rows]

    for n in range(1, na):
        complete(n)
        project(order[n])
        if n + 2 < na:
            share(n + 2)
        if n + 1 < na:
            hand_over(n + 1)
        combine(order[n - 1], False)
    acc = combine(a, True)
    for x in a_peers:
        arrived(in2.at[x], s2_s, s2_r.at[x])
        acc += in2[x].astype(F32)
    result = dot(acc.astype(BF16), wo[...]).astype(BF16)
    for y in range(ny):
        o3[y] = result[y * own:(y + 1) * own]
    for y in vy_peers:
        send(o3.at[y], in3.at[j], s3_s, s3_r.at[j], i, y)
    final = o3[j].astype(F32)
    for y in vy_peers:
        arrived(in3.at[y], s3_s, s3_r.at[y])
        final += in3[y].astype(F32)
    out[...] = final.astype(BF16)
    for copy in sent:
        copy.wait_send()


def shards(tokens, var_embed, query, key_weight, value_weight, out_weight, var_slot):
    slots, batch, patches, width = tokens.shape
    nx, ny = lax.axis_size("vx"), lax.axis_size("vy")
    heads = HEADS
    rows, na, group, own = width // ny, ny // CORES, patches // nx, patches // (nx * ny)
    nplane = nx * CORES
    dma = pltpu.SemaphoreType.DMA
    vmem = pltpu.VMEM
    result = pl.pallas_call(
        functools.partial(kernel, nx, ny, heads),
        out_shape=jax.ShapeDtypeStruct((own, width), BF16),
        in_specs=[pl.BlockSpec(memory_space=pl.ANY)] * 7,
        out_specs=pl.BlockSpec(memory_space=pltpu.VMEM),
        scratch_shapes=[
            vmem((slots, batch * patches, width), BF16),
            vmem(var_embed.shape, BF16),
            vmem((width,), BF16),
            vmem((rows, width), BF16),
            vmem((rows, width), BF16),
            vmem((1, var_slot.shape[0]), jnp.int32),
            dma((7,)),
            vmem((slots * patches, width), BF16),
            vmem((width, width), BF16),
            vmem((2, heads, rows), BF16),
            vmem((ny, 2, heads, rows), BF16),
            vmem((2, heads, width), BF16),
            vmem((slots * patches, heads), BF16),
            vmem((patches, 2 * heads), F32),
            vmem((nplane, group, 2 * heads), F32),
            vmem((group, 2 * heads), F32),
            vmem((na, group, 2 * heads), F32),
            vmem((na, nplane, group, rows), F32),
            vmem((na, nplane, group, rows), BF16),
            vmem((na, nplane, group, rows), BF16),
            vmem((na, group, rows), BF16),
            vmem((na, group, rows), BF16),
            vmem((ny, own, width), BF16),
            vmem((ny, own, width), BF16),
            dma, dma((ny,)),
            dma, dma((2, na, nx, na)),
            dma, dma,
            dma, dma((nplane,)),
            dma, dma((na,)),
            dma, dma((na, nplane)),
            dma, dma((na,)),
            dma, dma((ny,)),
        ],
        compiler_params=pltpu.CompilerParams(
            collective_id=0, has_side_effects=True, vmem_limit_bytes=60 * 1024 * 1024),
    )(
        tokens.reshape(slots, batch * patches, width), var_embed, query,
        key_weight, value_weight, out_weight, var_slot.reshape(1, -1),
    )
    return result.reshape(batch, -1, width)


def solution(mesh):
    placed = (
        P(("vx", "vy"), None, None, None),
        P(),
        P(),
        P("vy", None),
        P("vy", None),
        P("vy", None),
        P(),
    )
    return jax.shard_map(
        shards, mesh=mesh, in_specs=placed, out_specs=P(None, ("vx", "vy"), None), check_vma=False
    )
```
